128 devices in a mesh: pts: 32 (over y, z, core), grp: 4 (over x).
Axes of the slice: x: 4, y: 4, z: 4, core: 2. Of those that a mesh axis runs over, the one named last changes fastest.
Arguments:
- coords: float32 [3, 65536], P(None, ('pts', 'grp')), may hold values from 0 to 1, as said below
- observations: float32 [65536], P(('pts', 'grp')), may hold values from -18 to 18
- length_scales: float32 [3], replicated, may hold values from 0.3 to 1
- nugget: float32 [1], replicated, may hold values from 0.05 to 0.3
- fetch_table: int32 [128, 128, 11], P(('pts', 'grp')), may hold values from 0 to 511
- slot_of: int32 [30, 65536], P(None, ('pts', 'grp')), may hold values from 0 to 2943, as said below
Outputs:
- whitened: float32 [65536], P(('pts', 'grp'))
- neg_loglik: float32 [], replicated
The draws below stay inside these ranges and needn't reach their ends.
Inputs may be any that keep to these rules, and one draw needn't show every extreme that they name: `coords`: the points of the device of tile t and slab s have first coordinate in [t / 32, (t + 1) / 32) and time coordinate in [s / 4, (s + 1) / 4). `slot_of`: the 30 slots of one point are distinct. Slots below 1536 never point before the first tile or after the last one. Only the first 32 points of each device use slots of 1536 or more, and each of those slots is used at most once on its device; on every device some owner's 11 far slots are all used.
All inputs are finite; a program needn't handle non-finite values.
Results may differ from the reference program's by a relative error of at most 0.0003.
Values sent between devices are 32-bit elements; how exact they have to be, the bound alone decides.
A program may use at most 128 MiB of HBM per device.

```python
import math
import jax
import jax.numpy as jnp
from jax import lax

M = 30
P_DEV = 512
EARLY = 32
OWNERS = 128
NPTS = 65536
FCAP = 11
N_PTS = 32
N_GRP = 4


def draw_coords(key, part):
    device = jnp.arange(NPTS, dtype=jnp.int32) // P_DEV
    tile = (device // N_GRP).astype(jnp.float32)
    slab = (device % N_GRP).astype(jnp.float32)
    spread = jax.random.uniform(jax.random.fold_in(key, 21), (3, NPTS), jnp.float32, 0.0, 1.0)
    first = (tile + spread[0]) / N_PTS
    third = (slab + spread[2]) / N_GRP
    return jnp.stack([first, spread[1], third], axis=0)


def draw_observations(key, part):
    position = jnp.arange(NPTS, dtype=jnp.float32)
    slope = 1.0 + 2.0 * position / NPTS
    rough = jax.random.normal(jax.random.fold_in(key, 12), (NPTS,), jnp.float32)
    return jnp.clip(rough, -6.0, 6.0) * slope


def draw_slot_of(key, part):
    far_total = OWNERS * FCAP
    far_uses = EARLY * M
    series = jnp.arange(far_total, dtype=jnp.int32)
    owner_of = series // FCAP
    stride = P_DEV // (M + 1)

    def per_device(device):
        device_key = jax.random.fold_in(key, device)
        tile = device // N_GRP
        filled = (device + OWNERS // 2) % OWNERS
        noise = jax.random.randint(jax.random.fold_in(device_key, 1), (far_total,), 0, 4096, dtype=jnp.int32)
        score = jnp.where(owner_of == filled, series - far_total, noise * far_total + series)
        chosen = jnp.argsort(score, stable=True)[:far_uses].astype(jnp.int32) + 3 * P_DEV
        chosen = jax.random.permutation(jax.random.fold_in(device_key, 2), chosen)
        chosen = chosen.reshape(EARLY, M).T
        local = jnp.arange(P_DEV, dtype=jnp.int32)[None, :]
        jitter = jax.random.randint(jax.random.fold_in(device_key, 3), (M, P_DEV), 0, stride, dtype=jnp.int32)
        offsets = 1 + jnp.arange(M, dtype=jnp.int32)[:, None] * stride + jitter
        rows = (local + offsets) % P_DEV
        block = jax.random.randint(jax.random.fold_in(device_key, 4), (M, P_DEV), 0, 3, dtype=jnp.int32)
        block = jnp.where((tile == 0) & (block == 0), 1, block)
        block = jnp.where((tile == N_PTS - 1) & (block == 2), 1, block)
        near = block * P_DEV + rows
        return jnp.concatenate([chosen, near[:, EARLY:]], axis=1).astype(jnp.int32)
    blocks = lax.map(per_device, jnp.arange(OWNERS, dtype=jnp.int32))
    return jnp.transpose(blocks, (1, 0, 2)).reshape(M, NPTS)


def touch_ends(result, stream_key, least, high):
    dims = result.shape
    place = [jax.random.randint(jax.random.fold_in(stream_key, axis), (), 0, dims[axis]) for axis in range(len(dims))]
    result = result.at[tuple(place)].set(least)
    longest = dims.index(max(dims))
    place[longest] = (place[longest] + 1) % dims[longest]
    return result.at[tuple(place)].set(high)


def setup_inputs(seed: int = 0) -> dict:
    splits = jax.random.split(jax.random.key(seed), 7)
    coords = draw_coords(jax.random.fold_in(splits[6], 71), 0)
    observations = draw_observations(jax.random.fold_in(splits[6], 71), 0)
    length_scales = jnp.clip(jnp.exp(jax.random.uniform(splits[2], (3,), jnp.float32, math.log(0.3), math.log(1.0))), 0.3, 1.0)
    nugget = jnp.clip(jnp.exp(jax.random.uniform(splits[3], (1,), jnp.float32, math.log(0.05), math.log(0.3))), 0.05, 0.3)
    fetch_table = touch_ends(jax.random.randint(splits[4], (OWNERS, OWNERS, FCAP), 0, P_DEV), jax.random.fold_in(splits[4], 1), 0, P_DEV - 1).astype(jnp.int32)
    slot_of = draw_slot_of(jax.random.fold_in(splits[6], 71), 0)
    return {"coords": coords, "observations": observations, "length_scales": length_scales, "nugget": nugget, "fetch_table": fetch_table, "slot_of": slot_of}


root_three = 1.7320508075688772
half_log_tau = 0.9189385332046727

def covariance(points, inverse_lengths, nugget):
    scaled = points * inverse_lengths[:, None, None]
    gap = scaled[:, :, None, :] - scaled[:, None, :, :]
    distance = jnp.sqrt(lax.optimization_barrier(jnp.sum(gap * gap, axis=0)))
    scaled_distance = root_three * distance
    order = points.shape[1]
    identity = jnp.eye(order, dtype=jnp.float32)[:, :, None]
    return (1.0 + scaled_distance) * jnp.exp(-scaled_distance) + nugget[0] * identity

def eliminate(matrix, values):
    order = matrix.shape[0]
    for step in range(order):
        pivot = jnp.sqrt(matrix[0, 0])
        solved = values[0] / pivot
        if step == order - 1:
            return (solved, pivot)
        column = matrix[1:, 0] / pivot
        matrix = matrix[1:, 1:] - column[:, None, :] * column[None, :, :]
        values = values[1:] - column * solved

def reference(coords, observations, length_scales, nugget, fetch_table, slot_of):
    inverse_lengths = 1.0 / length_scales

    def per_device(device):
        table = lax.dynamic_index_in_dim(fetch_table, device, 0, keepdims=False)
        near_dev = jnp.clip(device + (jnp.arange(3, dtype=jnp.int32) - 1) * N_GRP, 0, OWNERS - 1)
        near_rows = (near_dev[:, None] * P_DEV + jnp.arange(P_DEV, dtype=jnp.int32)[None, :]).reshape(-1)
        far_rows = (jnp.arange(OWNERS, dtype=jnp.int32)[:, None] * P_DEV + table).reshape(-1)
        slot_rows = jnp.concatenate([near_rows, far_rows]).astype(jnp.int32)
        positions = lax.dynamic_slice_in_dim(slot_of, (device * P_DEV).astype(jnp.int32), P_DEV, 1)
        neighbours = slot_rows[positions]
        own_rows = (device * P_DEV + jnp.arange(P_DEV, dtype=jnp.int32))[None, :]
        members = jnp.concatenate([neighbours, own_rows], axis=0)
        points = coords[:, members]
        values = observations[members]
        matrix = covariance(points, inverse_lengths, nugget)
        solved, pivot = eliminate(matrix, values)
        return (solved, jnp.sum(2.0 * jnp.log(pivot) + solved * solved))
    whitened, partial_value = lax.map(per_device, jnp.arange(OWNERS, dtype=jnp.int32))
    neg_loglik = jnp.sum(partial_value) / (2.0 * NPTS) + half_log_tau
    return (whitened.reshape(NPTS), neg_loglik)
```

```python
import functools

import jax
import jax.numpy as jnp
from jax import lax
from jax.experimental import pallas as pl
from jax.experimental.pallas import tpu as pltpu
from jax.sharding import PartitionSpec as P

ALL = ("pts", "grp")
MESH = pl.DeviceIdType.MESH

root_three = 1.7320508075688772
half_log_tau = 0.9189385332046727

POINTS = 512
LANES = 128
CHUNKS = POINTS // LANES
ORDER = 31
CAP = 11
NEAR = 3 * POINTS
DEVICES = 128


def hops(offset):
    y, z, core, x = offset
    ring = (0, 1, 2, 1)
    return ring[y] + ring[z] + ring[x] + 0.3 * core


def far_first(offsets):
    return sorted(offsets, key=lambda offset: -hops(offset))


EVERYONE = far_first(
    (y, z, core, x)
    for y in range(4)
    for z in range(4)
    for core in range(2)
    for x in range(4)
    if (y, z, core, x) != (0, 0, 0, 0)
)
PLANE = [offset for offset in EVERYONE if offset[2:] == (0, 0)]
GROUP = [offset for offset in EVERYONE if offset[:2] == (0, 0)]


def spread(row, shape):
    return jnp.broadcast_to(row, shape)


def lanes_of(row, lane):
    return jnp.take_along_axis(
        spread(row, lane.shape), lane, axis=1, mode="promise_in_bounds"
    )


def eliminate(scaled, observed, nugget, held, eliminated, chunk_ref):
    coords, _ = held
    tile = (8, LANES)
    sub = lax.broadcasted_iota(jnp.int32, tile, 0)
    for panel in range(4):
        first = 8 * panel
        members = range(first, min(first + 8, ORDER))
        tiles = range(panel, 4)
        rows = {}
        for a in members:
            here = [spread(coords[c, a : a + 1, :], tile) for c in range(4)]
            for t in tiles:
                square = None
                for c in range(3):
                    gap = scaled[c][8 * t : 8 * t + 8] - here[c]
                    square = gap * gap if square is None else square + gap * gap
                square = jnp.maximum(square, 1e-36)
                distance = square * lax.rsqrt(square)
                value = (1.0 + distance) * jnp.exp(-distance)
                if t == panel:
                    value = jnp.where(sub == a - first, value + nugget, value)
                if t == 3:
                    value = jnp.where(sub == 7, here[3], value)
                rows[a, t] = value
        for k in range(first):
            column = {t: eliminated[k, t] for t in tiles}
            for a in members:
                factor = spread(eliminated[k, panel, a - first : a - first + 1, :], tile)
                for t in tiles:
                    rows[a, t] = rows[a, t] - factor * column[t]
        for k in members:
            pivot = rows[k, panel][k - first : k - first + 1, :]
            if k == ORDER - 1:
                solved = rows[k, 3][7:8, :] * lax.rsqrt(pivot)
                chunk_ref[...] = solved
                return jnp.log(pivot) + solved * solved
            inverse = lax.rsqrt(spread(pivot, tile))
            column = {t: rows[k, t] * inverse for t in tiles}
            for t in tiles:
                if t > panel:
                    eliminated[k, t] = column[t]
            for a in range(k + 1, members[-1] + 1):
                factor = spread(column[panel][a - first : a - first + 1, :], tile)
                for t in tiles:
                    rows[a, t] = rows[a, t] - factor * column[t]


def kernel(
    coords_hbm, obs_hbm, scales_hbm, nugget_hbm, fetch_hbm, slot_hbm,
    white_hbm, nll_hbm,
    coords, obs, fetch, slots, scales, nugget_s, held, eliminated, white, reply, far, part, reduced, nll,
    local_sem, group_send, group_recv, request_sem, reply_sem, reduce_sem, out_sem,
):
    pts, x = lax.axis_index("pts"), lax.axis_index("grp")
    s, core = pts // 2, pts % 2
    y, z = s // 4, s % 4
    me = 8 * s + 4 * core + x
    mine = 4 * core + x

    def device(offset):
        dy, dz, dcore, dx = offset
        return ((((y + dy) % 4) * 4 + (z + dz) % 4) * 2 + (core + dcore) % 2, (x + dx) % 4)

    across = ((((s + 2 * core + 15) % 16) * 2 + 1 - core), x)

    barrier = pltpu.get_barrier_semaphore()
    peers = [device(o) for o in PLANE] + [device(o) for o in GROUP] + [across]
    for peer in peers:
        pl.semaphore_signal(barrier, 1, device_id=peer, device_id_type=MESH)

    loads = [
        pltpu.make_async_copy(fetch_hbm, fetch.at[s], local_sem.at[0]),
        pltpu.make_async_copy(coords_hbm, coords.at[mine], local_sem.at[1]),
        pltpu.make_async_copy(obs_hbm, obs.at[mine], local_sem.at[2]),
        pltpu.make_async_copy(slot_hbm, slots, local_sem.at[3]),
        pltpu.make_async_copy(scales_hbm, scales, local_sem.at[4]),
        pltpu.make_async_copy(nugget_hbm, nugget_s, local_sem.at[5]),
    ]
    for load in loads:
        load.start()
    for load in loads:
        load.wait()
    pl.semaphore_wait(barrier, len(peers))

    def remote(src, dst, send, recv, peer):
        return pltpu.make_async_remote_copy(
            src_ref=src, dst_ref=dst, send_sem=send, recv_sem=recv, device_id=peer, device_id_type=MESH
        )

    for offset in PLANE:
        remote(fetch.at[s], fetch.at[s], request_sem.at[0], request_sem.at[1], device(offset)).start()
    for peer, slot in [(across, 8)] + [(device(o), mine) for o in GROUP]:
        remote(coords.at[mine], coords.at[slot], group_send.at[0], group_recv.at[slot, 0], peer).start()
        remote(obs.at[mine], obs.at[slot], group_send.at[1], group_recv.at[slot, 1], peer).start()

    def arrived(slot):
        pltpu.make_async_copy(coords.at[slot], coords.at[slot], group_recv.at[slot, 0]).wait()
        pltpu.make_async_copy(obs.at[slot], obs.at[slot], group_recv.at[slot, 1]).wait()

    def table_row(slot, c, block):
        if c == 3:
            return obs[slot, block : block + 1, :]
        return coords[slot, c : c + 1, block * LANES : (block + 1) * LANES]

    tile = (8, LANES)
    factor = [jnp.float32(root_three) / jnp.full((1, LANES), scales[c], jnp.float32) for c in range(3)]
    nugget = nugget_s[0]
    before = core * x + (1 - core) * 8
    after = core * 8 + (1 - core) * (4 + x)

    def near_rows(index):
        block, lane = index >> 7, index & 127
        found = [jnp.zeros(index.shape, jnp.float32) for _ in range(4)]
        for r in range(12):
            at = block == r
            slot = (before, mine, after)[r // 4]
            for c in range(4):
                found[c] = jnp.where(at, lanes_of(table_row(slot, c, r % 4), lane), found[c])
        return found

    def finish(found, chunk):
        scaled = [found[c] * factor[c] for c in range(3)]
        for c in range(3):
            held[c] = scaled[c]
        held[3] = found[3]
        return eliminate(scaled, found[3], nugget, (held, None), eliminated, white.at[pl.ds(chunk, 1), :])

    def index_of(chunk):
        itself = POINTS + chunk * LANES + lax.broadcasted_iota(jnp.int32, (2, LANES), 1)
        listed = slots[:, pl.ds(pl.multiple_of(chunk * LANES, LANES), LANES)]
        return jnp.concatenate([listed, itself], axis=0)

    def near_chunk(chunk, total):
        return total + finish(near_rows(index_of(chunk)), chunk)

    arrived((1 - core) * 4 + x)
    arrived(8)
    total = near_chunk(1, jnp.zeros((1, LANES), jnp.float32))

    for offset in GROUP:
        _, _, dcore, dx = offset
        if (dcore, dx) != (1, 0):
            arrived(((core + dcore) % 2) * 4 + (x + dx) % 4)
    pltpu.make_async_copy(fetch.at[pl.ds(0, 15)], fetch.at[pl.ds(0, 15)], request_sem.at[1]).wait()
    lane_id = lax.broadcasted_iota(jnp.int32, (16, LANES), 1)
    wanted = jnp.zeros((16, LANES), jnp.int32)
    for q in range(16):
        asked = jnp.concatenate([fetch[q], jnp.zeros((5, LANES), jnp.int32)], axis=0)
        asked = pltpu.roll(asked, (8 * q - 8 * s + LANES) % LANES, axis=1)
        wanted = jnp.where(lane_id // 8 == q, asked, wanted)
    owner_block, lane = (lane_id % 8) * 4 + (wanted >> 7), wanted & 127
    served = [jnp.zeros((16, LANES), jnp.float32) for _ in range(4)]
    for r in range(32):
        at = owner_block == r
        for c in range(4):
            served[c] = jnp.where(at, lanes_of(table_row(r // 4, c, r % 4), lane), served[c])
    stacked = jnp.concatenate(served + [jnp.zeros((64, LANES), jnp.float32)], axis=0)
    reply[...] = stacked.T
    far[pl.ds(pl.multiple_of(8 * s, 8), 8), :] = reply[pl.ds(pl.multiple_of(8 * s, 8), 8), :]
    for offset in PLANE:
        peer = device(offset)
        there = peer[0] // 2
        remote(
            reply.at[pl.ds(pl.multiple_of(8 * there, 8), 8), :],
            far.at[pl.ds(pl.multiple_of(8 * s, 8), 8), :],
            reply_sem.at[0], reply_sem.at[1], peer,
        ).start()

    total = lax.fori_loop(2, CHUNKS, near_chunk, total)
    index = index_of(0)
    found = near_rows(index)

    pltpu.make_async_copy(far.at[pl.ds(0, 120)], far.at[pl.ds(0, 120)], reply_sem.at[1]).wait()
    table = far[...].T
    number = index - NEAR
    owner = (number * 5958) >> 16
    place = jnp.where(number >= 0, number - CAP * owner, -1)
    owner = owner & 127
    for r in range(CAP):
        at = place == r
        for c in range(4):
            row = table[16 * c + r : 16 * c + r + 1, :]
            found[c] = jnp.where(at, lanes_of(row, owner), found[c])
    total = total + finish(found, 0)

    out = pltpu.make_async_copy(white, white_hbm, out_sem.at[0])
    out.start()
    part[0] = total
    reduced[me] = total
    for offset in EVERYONE:
        remote(part.at[0], reduced.at[me], reduce_sem.at[0], reduce_sem.at[1], device(offset)).start()
    pltpu.make_async_copy(reduced.at[pl.ds(0, 127)], reduced.at[pl.ds(0, 127)], reduce_sem.at[1]).wait()
    everything = jnp.sum(reduced[...], axis=0)
    scale = 1.0 / (2.0 * POINTS * DEVICES)
    nll[...] = jnp.full((1, LANES), jnp.sum(everything) * scale + half_log_tau, jnp.float32)
    nll_out = pltpu.make_async_copy(nll, nll_hbm, out_sem.at[1])
    nll_out.start()

    pltpu.make_async_copy(fetch.at[pl.ds(0, 15)], fetch.at[pl.ds(0, 15)], request_sem.at[0]).wait()
    pltpu.make_async_copy(coords.at[pl.ds(0, 8)], coords.at[pl.ds(0, 8)], group_send.at[0]).wait()
    pltpu.make_async_copy(obs.at[pl.ds(0, 8)], obs.at[pl.ds(0, 8)], group_send.at[1]).wait()
    pltpu.make_async_copy(far.at[pl.ds(0, 120)], far.at[pl.ds(0, 120)], reply_sem.at[0]).wait()
    pltpu.make_async_copy(reduced.at[pl.ds(0, 127)], reduced.at[pl.ds(0, 127)], reduce_sem.at[0]).wait()
    out.wait()
    nll_out.wait()


def body(coords, observations, length_scales, nugget, fetch_table, slot_of):
    anywhere = pl.BlockSpec(memory_space=pl.ANY)
    white, nll = pl.pallas_call(
        kernel,
        out_shape=(
            jax.ShapeDtypeStruct((CHUNKS, LANES), jnp.float32),
            jax.ShapeDtypeStruct((1, LANES), jnp.float32),
        ),
        in_specs=[anywhere] * 6,
        out_specs=(anywhere, anywhere),
        scratch_shapes=[
            pltpu.VMEM((9, 3, POINTS), jnp.float32),
            pltpu.VMEM((9, CHUNKS, LANES), jnp.float32),
            pltpu.VMEM((16, CAP, LANES), jnp.int32),
            pltpu.VMEM((ORDER - 1, POINTS), jnp.int32),
            pltpu.SMEM((3,), jnp.float32),
            pltpu.SMEM((1,), jnp.float32),
            pltpu.VMEM((4, 32, LANES), jnp.float32),
            pltpu.VMEM((ORDER, 4, 8, LANES), jnp.float32),
            pltpu.VMEM((CHUNKS, LANES), jnp.float32),
            pltpu.VMEM((128, LANES), jnp.float32),
            pltpu.VMEM((128, LANES), jnp.float32),
            pltpu.VMEM((1, 1, LANES), jnp.float32),
            pltpu.VMEM((DEVICES, 1, LANES), jnp.float32),
            pltpu.VMEM((1, LANES), jnp.float32),
            pltpu.SemaphoreType.DMA((6,)),
            pltpu.SemaphoreType.DMA((2,)),
            pltpu.SemaphoreType.DMA((9, 2)),
            pltpu.SemaphoreType.DMA((2,)),
            pltpu.SemaphoreType.DMA((2,)),
            pltpu.SemaphoreType.DMA((2,)),
            pltpu.SemaphoreType.DMA((2,)),
        ],
        compiler_params=pltpu.CompilerParams(collective_id=0, has_side_effects=True),
        name="vecchia",
    )(
        coords,
        observations.reshape(CHUNKS, LANES),
        length_scales,
        nugget,
        jnp.transpose(fetch_table, (2, 0, 1)).reshape(CAP, LANES),
        slot_of,
    )
    return white.reshape(POINTS), nll[0, 0]


def solution(mesh):
    return jax.shard_map(
        body,
        mesh=mesh,
        in_specs=(P(None, ALL), P(ALL), P(), P(), P(ALL, None, None), P(None, ALL)),
        out_specs=(P(ALL), P()),
        check_vma=False,
    )
```

```python
import jax
import jax.numpy as jnp
from jax import lax
from jax.experimental import pallas as pl
from jax.experimental.pallas import tpu as pltpu
from jax.sharding import PartitionSpec as P

ALL = ("pts", "grp")
MESH = pl.DeviceIdType.MESH

root_three = 1.7320508075688772
half_log_tau = 0.9189385332046727

POINTS = 512
LANES = 128
CHUNKS = POINTS // LANES
ORDER = 31
CAP = 11
EARLY = 32
NEAR = 3 * POINTS
DEVICES = 128
TILE = (8, LANES)


def hops(offset):
    y, z, core, x = offset
    ring = (0, 1, 2, 1)
    return ring[y] + ring[z] + ring[x] + 0.3 * core


EVERYONE = sorted(
    (
        (y, z, core, x)
        for y in range(4)
        for z in range(4)
        for core in range(2)
        for x in range(4)
        if (y, z, core, x) != (0, 0, 0, 0)
    ),
    key=lambda offset: -hops(offset),
)
PLANE = [offset for offset in EVERYONE if offset[2:] == (0, 0)]
GROUP = [offset for offset in EVERYONE if offset[:2] == (0, 0)]


def spread(row, shape):
    return jnp.broadcast_to(row, shape)


def lanes_of(rows, lane):
    return jnp.take_along_axis(spread(rows, lane.shape), lane, axis=1, mode="promise_in_bounds")


def eliminate(scaled, nugget, held, eliminated, white_ref):
    sub = lax.broadcasted_iota(jnp.int32, TILE, 0)
    for panel in range(4):
        first = 8 * panel
        members = range(first, min(first + 8, ORDER))
        tiles = range(panel, 4)
        rows = {}
        for a in members:
            here = [spread(held[c, a : a + 1, :], TILE) for c in range(4)]
            for t in tiles:
                square = None
                for c in range(3):
                    gap = scaled[c][8 * t : 8 * t + 8] - here[c]
                    square = gap * gap if square is None else square + gap * gap
                square = jnp.maximum(square, 1e-36)
                distance = square * lax.rsqrt(square)
                value = (1.0 + distance) * jnp.exp(-distance)
                if t == panel:
                    value = jnp.where(sub == a - first, value + nugget, value)
                if t == 3:
                    value = jnp.where(sub == 7, here[3], value)
                rows[a, t] = value
        for k in range(first):
            column = {t: eliminated[k, t] for t in tiles}
            for a in members:
                factor = spread(eliminated[k, panel, a - first : a - first + 1, :], TILE)
                for t in tiles:
                    rows[a, t] = rows[a, t] - factor * column[t]
        for k in members:
            pivot = rows[k, panel][k - first : k - first + 1, :]
            if k == ORDER - 1:
                solved = rows[k, 3][7:8, :] * lax.rsqrt(pivot)
                white_ref[...] = solved
                return jnp.log(pivot) + solved * solved
            inverse = lax.rsqrt(spread(pivot, TILE))
            column = {t: rows[k, t] * inverse for t in tiles}
            for t in tiles:
                if t > panel:
                    eliminated[k, t] = column[t]
            for a in range(k + 1, members[-1] + 1):
                factor = spread(column[panel][a - first : a - first + 1, :], TILE)
                for t in tiles:
                    rows[a, t] = rows[a, t] - factor * column[t]


def kernel(
    coords_hbm, obs_hbm, scales_hbm, nugget_hbm, fetch_hbm, slot_hbm,
    white, sums,
    coords, obs, fetch, slots, scales, nugget_s,
    table, looked, asks, asked, answers, far, held, eliminated, part, reduced,
    local_sem, group_send, group_recv, request_sem, reply_sem, reduce_sem,
):
    pts, x = lax.axis_index("pts"), lax.axis_index("grp")
    s, core = pts // 2, pts % 2
    y, z = s // 4, s % 4
    me = 8 * s + 4 * core + x
    mine = 4 * core + x

    def device(offset):
        dy, dz, dcore, dx = offset
        return ((((y + dy) % 4) * 4 + (z + dz) % 4) * 2 + (core + dcore) % 2, (x + dx) % 4)

    across = ((((s + 2 * core + 15) % 16) * 2 + 1 - core), x)

    barrier = pltpu.get_barrier_semaphore()
    peers = [device(o) for o in PLANE] + [device(o) for o in GROUP] + [across]
    for peer in peers:
        pl.semaphore_signal(barrier, 1, device_id=peer, device_id_type=MESH)

    loads = [
        pltpu.make_async_copy(fetch_hbm.at[:, 0, :], fetch, local_sem.at[0]),
        pltpu.make_async_copy(coords_hbm, coords, local_sem.at[1]),
        pltpu.make_async_copy(obs_hbm, obs, local_sem.at[2]),
        pltpu.make_async_copy(slot_hbm, slots, local_sem.at[3]),
        pltpu.make_async_copy(scales_hbm, scales, local_sem.at[4]),
        pltpu.make_async_copy(nugget_hbm, nugget_s, local_sem.at[5]),
    ]
    for load in loads:
        load.start()
    for load in loads:
        load.wait()

    def strip(index):
        return pl.ds(pl.multiple_of(8 * index, 8), 8)

    line = lax.broadcasted_iota(jnp.int32, (LANES, LANES), 0)
    sixteen = jnp.concatenate([fetch[...], jnp.zeros((5, LANES), jnp.int32)], axis=0)
    asks[...] = jnp.where(line // 64 == s % 2, jnp.concatenate([sixteen] * 8, axis=0), 0).T
    for c in range(4):
        for b in range(CHUNKS):
            if c == 3:
                table[c, b, mine] = obs[b : b + 1, :]
            else:
                table[c, b, mine] = coords[c : c + 1, b * LANES : (b + 1) * LANES]
    asked[strip(s), :] = asks[strip(s), :]
    pl.semaphore_wait(barrier, len(peers))

    def remote(src, dst, send, recv, peer):
        return pltpu.make_async_remote_copy(
            src_ref=src, dst_ref=dst, send_sem=send, recv_sem=recv, device_id=peer, device_id_type=MESH
        )

    for slot, peer in [(mine, device(o)) for o in GROUP] + [(8, across)]:
        remote(table.at[:, :, mine], table.at[:, :, slot], group_send, group_recv.at[slot], peer).start()
    for offset in PLANE:
        peer = device(offset)
        remote(
            asks.at[strip(peer[0] // 2), :], asked.at[strip(s), :],
            request_sem.at[0], request_sem.at[1], peer,
        ).start()

    def index_of(chunk):
        itself = POINTS + chunk * LANES + lax.broadcasted_iota(jnp.int32, (2, LANES), 1)
        listed = slots[:, pl.ds(pl.multiple_of(chunk * LANES, LANES), LANES)]
        return jnp.concatenate([listed, itself], axis=0)

    def look_up(index, found, tiles):
        block, lane = index >> 7, index & 127
        for which, slot in tiles:
            for b in range(CHUNKS):
                at = block == CHUNKS * which + b
                for c in range(4):
                    found[c] = jnp.where(at, lanes_of(table[c, b, slot], lane), found[c])
        return found

    def own_rows(chunk, carry):
        found = look_up(index_of(chunk), [jnp.zeros((32, LANES), jnp.float32)] * 4, [(1, mine)])
        for c in range(4):
            looked[chunk, c] = found[c]
        return carry

    lax.fori_loop(0, CHUNKS, own_rows, 0)

    def arrived(slot):
        pltpu.make_async_copy(table.at[:, :, slot], table.at[:, :, slot], group_recv.at[slot]).wait()

    for offset in GROUP:
        _, _, dcore, dx = offset
        arrived(((core + dcore) % 2) * 4 + (x + dx) % 4)
    pltpu.make_async_copy(asked.at[pl.ds(0, 120)], asked.at[pl.ds(0, 120)], request_sem.at[1]).wait()

    owned = [table[r // 4, r % 4, 0:8, 0, :] for r in range(16)]
    part_of = (lax.broadcasted_iota(jnp.int32, TILE, 1) // 16 % 4) * 4
    for p in range(8):
        wanted = asked[16 * p : 16 * p + 8, :] + asked[16 * p + 8 : 16 * p + 16, :]
        key, lane = part_of + (wanted >> 7), wanted & 127
        served = jnp.zeros(TILE, jnp.float32)
        for r in range(16):
            served = jnp.where(key == r, lanes_of(owned[r], lane), served)
        answers[8 * p : 8 * p + 8, :] = served
    far[strip(s), :] = answers[strip(s // 2), :]
    for offset in PLANE:
        peer = device(offset)
        remote(
            answers.at[strip(peer[0] // 4), :], far.at[strip(s), :],
            reply_sem.at[0], reply_sem.at[1], peer,
        ).start()

    factor = [jnp.float32(root_three) / jnp.full((1, LANES), scales[c], jnp.float32) for c in range(3)]
    nugget = nugget_s[0]
    before = core * x + (1 - core) * 8
    after = core * 8 + (1 - core) * (4 + x)

    def near_rows(chunk):
        return look_up(index_of(chunk), [looked[chunk, c] for c in range(4)], [(0, before), (2, after)])

    def finish(found, chunk):
        scaled = [found[c] * factor[c] for c in range(3)]
        for c in range(3):
            held[c] = scaled[c]
        held[3] = found[3]
        return eliminate(scaled, nugget, held, eliminated, white.at[pl.ds(chunk, 1), :])

    def near_chunk(chunk, total):
        return total + finish(near_rows(chunk), chunk)

    arrived(8)
    total = lax.fori_loop(1, CHUNKS, near_chunk, jnp.zeros((1, LANES), jnp.float32))

    found = near_rows(0)
    number = index_of(0) - NEAR
    lane_id = lax.broadcasted_iota(jnp.int32, TILE, 1)
    packed = number[0:8]
    for t in range(1, 4):
        packed = jnp.where(lane_id // EARLY == t, pltpu.roll(number[8 * t : 8 * t + 8], EARLY * t, axis=1), packed)
    owner = (packed * 5958) >> 16
    place = jnp.where(packed >= 0, packed - CAP * owner, -1)
    owner = owner & 127
    is_far = [(number[8 * t : 8 * t + 8] >= 0) & (lane_id < EARLY) for t in range(4)]

    pltpu.make_async_copy(far.at[pl.ds(0, 120)], far.at[pl.ds(0, 120)], reply_sem.at[1]).wait()
    turned = far[...].T
    turned = jnp.where(s % 2 == 1, turned[64:128], turned[0:64])
    for c in range(4):
        fetched = jnp.zeros(TILE, jnp.float32)
        for r in range(CAP):
            fetched = jnp.where(place == r, lanes_of(turned[16 * c + r : 16 * c + r + 1, :], owner), fetched)
        found[c] = jnp.concatenate(
            [
                jnp.where(
                    is_far[t],
                    pltpu.roll(fetched, LANES - EARLY * t, axis=1) if t else fetched,
                    found[c][8 * t : 8 * t + 8],
                )
                for t in range(4)
            ],
            axis=0,
        )
    total = total + finish(found, 0)

    part[0] = total
    reduced[me] = total
    for offset in EVERYONE:
        remote(part.at[0], reduced.at[me], reduce_sem.at[0], reduce_sem.at[1], device(offset)).start()

    pltpu.make_async_copy(table.at[:, :, pl.ds(0, 8)], table.at[:, :, pl.ds(0, 8)], group_send).wait()
    pltpu.make_async_copy(asked.at[pl.ds(0, 120)], asked.at[pl.ds(0, 120)], request_sem.at[0]).wait()
    pltpu.make_async_copy(far.at[pl.ds(0, 120)], far.at[pl.ds(0, 120)], reply_sem.at[0]).wait()
    pltpu.make_async_copy(reduced.at[pl.ds(0, 127)], reduced.at[pl.ds(0, 127)], reduce_sem.at[1]).wait()
    sums[...] = jnp.sum(reduced[...], axis=0)
    pltpu.make_async_copy(reduced.at[pl.ds(0, 127)], reduced.at[pl.ds(0, 127)], reduce_sem.at[0]).wait()


def closing(white, sums, white_hbm, nll_hbm, nll, sem):
    out = pltpu.make_async_copy(white, white_hbm, sem.at[0])
    out.start()
    scale = 1.0 / (2.0 * POINTS * DEVICES)
    nll[...] = jnp.sum(sums[...], axis=1, keepdims=True) * scale + half_log_tau
    nll_out = pltpu.make_async_copy(nll, nll_hbm, sem.at[1])
    nll_out.start()
    out.wait()
    nll_out.wait()


def body(coords, observations, length_scales, nugget, fetch_table, slot_of):
    hbm = pl.BlockSpec(memory_space=pltpu.HBM)
    vmem = pl.BlockSpec(memory_space=pltpu.VMEM)
    white, sums = pl.pallas_call(
        kernel,
        out_shape=(pltpu.VMEM((CHUNKS, LANES), jnp.float32), pltpu.VMEM((1, LANES), jnp.float32)),
        in_specs=[hbm] * 6,
        out_specs=(vmem, vmem),
        scratch_shapes=[
            pltpu.VMEM((3, POINTS), jnp.float32),
            pltpu.VMEM((CHUNKS, LANES), jnp.float32),
            pltpu.VMEM((CAP, LANES), jnp.int32),
            pltpu.VMEM((ORDER - 1, POINTS), jnp.int32),
            pltpu.SMEM((3,), jnp.float32),
            pltpu.SMEM((1,), jnp.float32),
            pltpu.VMEM((4, CHUNKS, 9, 1, LANES), jnp.float32),
            pltpu.VMEM((CHUNKS, 4, 32, LANES), jnp.float32),
            pltpu.VMEM((LANES, LANES), jnp.int32),
            pltpu.VMEM((LANES, LANES), jnp.int32),
            pltpu.VMEM((64, LANES), jnp.float32),
            pltpu.VMEM((LANES, LANES), jnp.float32),
            pltpu.VMEM((4, 32, LANES), jnp.float32),
            pltpu.VMEM((ORDER, 4, 8, LANES), jnp.float32),
            pltpu.VMEM((1, 1, LANES), jnp.float32),
            pltpu.VMEM((DEVICES, 1, LANES), jnp.float32),
            pltpu.SemaphoreType.DMA((6,)),
            pltpu.SemaphoreType.DMA,
            pltpu.SemaphoreType.DMA((9,)),
            pltpu.SemaphoreType.DMA((2,)),
            pltpu.SemaphoreType.DMA((2,)),
            pltpu.SemaphoreType.DMA((2,)),
        ],
        compiler_params=pltpu.CompilerParams(collective_id=0, has_side_effects=True),
        name="vecchia",
    )(
        coords,
        observations.reshape(CHUNKS, LANES),
        length_scales,
        nugget,
        jnp.transpose(fetch_table, (2, 0, 1)),
        slot_of,
    )
    white, nll = pl.pallas_call(
        closing,
        out_shape=(
            jax.ShapeDtypeStruct((CHUNKS, LANES), jnp.float32),
            jax.ShapeDtypeStruct((1, 1), jnp.float32),
        ),
        in_specs=[vmem, vmem],
        out_specs=(hbm, hbm),
        scratch_shapes=[pltpu.VMEM((1, 1), jnp.float32), pltpu.SemaphoreType.DMA((2,))],
        name="closing",
    )(pltpu.with_memory_space_constraint(white, pltpu.VMEM), pltpu.with_memory_space_constraint(sums, pltpu.VMEM))
    return white.reshape(POINTS), nll.reshape(())


def solution(mesh):
    return jax.shard_map(
        body,
        mesh=mesh,
        in_specs=(P(None, ALL), P(ALL), P(), P(), P(ALL, None, None), P(None, ALL)),
        out_specs=(P(ALL), P()),
        check_vma=False,
    )
```
